32 devices in a mesh: tm: 4 (over y, x), space: 8 (over z, core).
Axes of the slice: x: 2, y: 2, z: 4, core: 2. Of those that a mesh axis runs over, the one named last changes fastest.
Arguments:
- source: float32 [8, 1024, 5, 128], P('tm', 'space'), may hold values from -6 to 6
- terminal: float32 [1024, 5, 128], P('space'), may hold values from -6 to 6
- jacobian: float32 [4, 1024, 5, 5, 128], P('tm', 'space')
- face_coef: float32 [1024, 6, 128], P('space'), may hold values from 0.1 to 0.5
- cell_coef: float32 [1024, 128], P('space'), may hold values from 0.1 to 0.5
- neighbours: int32 [1024, 6], P('space'), may hold values from 0 to 160, as said below
- send_blocks: int32 [8, 2, 16], P('space'), may hold values from 0 to 127, as said below
- live_count: int32 [8], P('space'), may hold values from 64 to 128, as said below
- volume: float32 [1024, 128], P('space'), may hold values from 0.5 to 2
- shape_field: float32 [1024, 5, 128], P('space'), may hold values from -6 to 6
- weights: float32 [8], P('tm'), may hold values from 0.25 to 4
Outputs:
- adjoint: float32 [8, 1024, 5, 128], P('tm', 'space')
- sensitivity: float32 [1024], P('space')
The draws below stay inside these ranges and needn't reach their ends.
Inputs may be any that keep to these rules, and one draw needn't show every extreme that they name: `live_count`: some device has 128 live blocks in every draw. `send_blocks`: each index names a live block of its own device. `neighbours`: a slot below 128 names a live block of the same device; 128 to 159 name received blocks, those of the lower device first; 160 is an empty slot.
All inputs are finite; a program needn't handle non-finite values.
Results may differ from the reference program's by a relative error of at most 0.00016.
Values sent between devices are 32-bit elements; how exact they have to be, the bound alone decides.
A program may use at most 64 MiB of HBM per device.

```python
import math
import jax
import jax.numpy as jnp
from jax import lax

NB = 128
CELLS = 128
COMP = 5
NEI = 6
HALO = 16
STEPS = 2
ITERS = 3
BLOCKS = 1024
GROUPS = 4
TSTEPS = 8
N_SPACE = 8


def geometry(key):
    devices = BLOCKS // NB
    keys = jax.random.split(jax.random.fold_in(key, 17), 6)
    counts = jax.random.randint(keys[0], (devices,), NB // 2, NB + 1)
    fullest = jax.random.randint(keys[1], (), 0, devices)
    counts = counts.at[fullest].set(NB)
    sends = jax.random.randint(keys[2], (devices, 2, HALO), 0, 1 << 20) % counts[:, None, None]
    kinds = jax.random.randint(keys[3], (BLOCKS, NEI), 0, 6)
    block_counts = jnp.repeat(counts, NB)
    local = jax.random.randint(keys[4], (BLOCKS, NEI), 0, 1 << 20) % block_counts[:, None]
    remote = NB + jax.random.randint(keys[5], (BLOCKS, NEI), 0, 2 * HALO)
    table = jnp.where(kinds < 2, remote, jnp.where(kinds == 2, NB + 2 * HALO, local))
    return (counts.astype(jnp.int32), sends.astype(jnp.int32), table.astype(jnp.int32))


def draw_live_count(key, part):
    return geometry(key)[0]


def draw_send_blocks(key, part):
    return geometry(key)[1]


def draw_neighbours(key, part):
    return geometry(key)[2]


def draw_jacobian(key, part):
    first, second = jax.random.split(jax.random.fold_in(key, 29))
    shape = (GROUPS, BLOCKS, COMP, COMP, CELLS)
    identity = jnp.eye(COMP, dtype=jnp.float32)[None, None, :, :, None]
    off_part = 0.15 * jax.random.normal(first, shape, jnp.float32)
    diag_part = jax.random.uniform(second, shape, jnp.float32, 0.3, 1.0)
    return identity * diag_part + (1.0 - identity) * off_part


def block_scale(stream_key, shape, shards, smallest, top_value):
    gain, own = 1.0, jax.random.fold_in(stream_key, 6)
    for dim, shards_of in shards:
        draws = jnp.exp(jax.random.uniform(jax.random.fold_in(own, dim), (shards_of,), jnp.float32, smallest / len(shards), top_value / len(shards)))
        gain = gain * jnp.repeat(draws, shape[dim] // shards_of).reshape([-1 if axis == dim else 1 for axis in range(len(shape))])
    return gain


def scatter_about(stream_key, dims, spread, limit, cuts=(), kind=jnp.bfloat16):
    entries = spread * jax.random.normal(stream_key, dims, jnp.float32)
    if cuts:
        entries = entries * block_scale(stream_key, dims, cuts, -0.22, 0.18)
    return jnp.clip(entries, -limit, limit).astype(kind)


def setup_inputs(seed: int = 0) -> dict:
    arg_keys = jax.random.split(jax.random.key(seed), 12)
    source = scatter_about(arg_keys[0], (TSTEPS, BLOCKS, COMP, CELLS), 1.0, 6.0, ((0, 4), (1, 8)), jnp.float32)
    terminal = scatter_about(arg_keys[1], (BLOCKS, COMP, CELLS), 1.0, 6.0, ((0, 8),), jnp.float32)
    jacobian = draw_jacobian(jax.random.fold_in(arg_keys[11], 71), 0)
    face_coef = jnp.clip(0.1 + 0.4 * jax.random.uniform(arg_keys[3], (BLOCKS, NEI, CELLS), jnp.float32) ** block_scale(arg_keys[3], (BLOCKS, NEI, CELLS), ((0, 8),), -0.2, 0.2), 0.1, 0.5)
    cell_coef = jnp.clip(0.1 + 0.4 * jax.random.uniform(arg_keys[4], (BLOCKS, CELLS), jnp.float32) ** block_scale(arg_keys[4], (BLOCKS, CELLS), ((0, 8),), -0.2, 0.2), 0.1, 0.5)
    neighbours = draw_neighbours(jax.random.fold_in(arg_keys[11], 71), 0)
    send_blocks = draw_send_blocks(jax.random.fold_in(arg_keys[11], 71), 0)
    live_count = draw_live_count(jax.random.fold_in(arg_keys[11], 71), 0)
    volume = jnp.clip(jnp.exp(math.log(2.0) - 1.3862944 * jax.random.uniform(arg_keys[8], (BLOCKS, CELLS), jnp.float32) ** block_scale(arg_keys[8], (BLOCKS, CELLS), ((0, 8),), -0.2, 0.2)), 0.5, 2.0)
    shape_field = scatter_about(arg_keys[9], (BLOCKS, COMP, CELLS), 1.0, 6.0, ((0, 8),), jnp.float32)
    weights = jnp.clip(jnp.exp(math.log(4.0) - 2.7725887 * jax.random.uniform(arg_keys[10], (TSTEPS,), jnp.float32) ** block_scale(arg_keys[10], (TSTEPS,), ((0, 4),), -0.2, 0.2)), 0.25, 4.0)
    return {"source": source, "terminal": terminal, "jacobian": jacobian, "face_coef": face_coef, "cell_coef": cell_coef, "neighbours": neighbours, "send_blocks": send_blocks, "live_count": live_count, "volume": volume, "shape_field": shape_field, "weights": weights}


inverse_step = 6.0


def pick_rows(table, index):
    return table[index]


def reference(source, terminal, jacobian, face_coef, cell_coef, neighbours, send_blocks, live_count, volume, shape_field, weights):
    highest = lax.Precision.HIGHEST
    live = (jnp.arange(NB, dtype=jnp.int32)[None, :] < live_count[:, None]).astype(jnp.float32).reshape(BLOCKS, 1, 1)
    mass = (inverse_step * volume)[:, None, :]
    face_total = jnp.sum(face_coef, axis=1)[:, None, :]
    along_coef = cell_coef[:, None, :]
    neighbour_table = neighbours.reshape(N_SPACE, NB, NEI)

    def operate(field, jac):
        by_device = field.reshape(N_SPACE, NB, COMP, CELLS)
        to_lower = jax.vmap(pick_rows)(by_device, send_blocks[:, 0])
        to_higher = jax.vmap(pick_rows)(by_device, send_blocks[:, 1])
        zero_rim = jnp.zeros((1, HALO, COMP, CELLS), jnp.float32)
        from_lower = jnp.concatenate([zero_rim, to_higher[:-1]], axis=0)
        from_higher = jnp.concatenate([to_lower[1:], zero_rim], axis=0)
        blank = jnp.zeros((N_SPACE, 1, COMP, CELLS), jnp.float32)
        extended = jnp.concatenate([by_device, from_lower, from_higher, blank], axis=1)
        gathered = jax.vmap(pick_rows)(extended, neighbour_table).reshape(BLOCKS, NEI, COMP, CELLS)
        coupled = jnp.einsum("bnc,bnkc->bkc", face_coef, gathered, precision=highest)
        own = jnp.einsum("bijc,bic->bjc", jac, field, precision=highest)
        padded = jnp.pad(field, ((0, 0), (0, 0), (1, 1)))
        beside = padded[:, :, :-2] + padded[:, :, 2:]
        return mass * field + own - coupled - along_coef * beside

    later = live * terminal
    levels = []
    sensitivity = jnp.zeros((BLOCKS,), jnp.float32)
    for group in reversed(range(GROUPS)):
        jac = jacobian[group]
        diagonal = jnp.stack([jac[:, k, k, :] for k in range(COMP)], axis=1)
        precond = 1.0 / (mass + diagonal + face_total + 2.0 * along_coef)
        for level in reversed(range(STEPS)):
            index = group * STEPS + level
            rhs = source[index] + mass * later
            field = later
            for sweep in range(ITERS):
                field = live * (field + precond * (rhs - operate(field, jac)))
            levels.append(field)
            sensitivity = sensitivity + weights[index] * jnp.sum(field * shape_field, axis=(1, 2))
            later = field
    adjoint = jnp.stack(levels[::-1], axis=0)
    return adjoint, sensitivity
```

```python
import functools

import jax
import jax.numpy as jnp
from jax import lax
from jax.experimental import pallas as pl
from jax.experimental.pallas import tpu as pltpu
from jax.sharding import PartitionSpec as P

ITERS = 3
INVERSE_STEP = 6.0
TILE = 16
HIGHEST = lax.Precision.HIGHEST


def rows_at(start):
    return pl.ds(start if isinstance(start, int) else pl.multiple_of(start, TILE), TILE)


def split(x):
    high = x.astype(jnp.bfloat16)
    return high, (x - high.astype(jnp.float32)).astype(jnp.bfloat16)


def matmul(a, b, precision=None):
    return jnp.dot(a, b, precision=precision, preferred_element_type=jnp.float32)


def kernel(
    groups,
    width,
    source_hbm,
    terminal_hbm,
    jac_hbm,
    face_hbm,
    cell_hbm,
    nbr_hbm,
    send_blocks,
    live_count,
    volume_hbm,
    shape_hbm,
    weights,
    adjoint_hbm,
    sens_ref,
    source,
    terminal,
    jac,
    face,
    cell,
    nbr,
    volume,
    shape,
    field,
    part,
    rate,
    rate_mass,
    cell_left,
    cell_right,
    rhs,
    levels,
    weighted,
    near_pick,
    far_pick,
    field_terms,
    part_terms,
    halo_terms,
    edge_terms,
    near,
    far,
    select,
    select_terms,
    own_fixed,
    own_rate,
    their_fixed,
    their_rate,
    their_pick,
    edge_halo,
    from_partner,
    from_across,
    from_second,
    edge_out,
    part_out,
    acc_in,
    acc_out,
    total,
    load_sem,
    store_sem,
    copy_send,
    copy_recv,
    coef_send,
    coef_recv,
    partner_send,
    partner_recv,
    across_send,
    across_recv,
    second_send,
    second_recv,
    first_send,
    state_send,
    state_recv,
    acc_send,
    acc_recv,
    total_send,
    total_recv,
):
    g = lax.axis_index("tm")
    d = lax.axis_index("space")
    _, steps, comp, nb, cells = source.shape
    nei = face.shape[0]
    count = edge_out.shape[3]
    sweeps = steps * ITERS
    tiles = nb // TILE
    edges = 2 * count
    top = groups - 1

    odd = lax.rem(d, 2)
    partner = d + 1 - 2 * odd
    across = d - 1 + 2 * odd
    beyond = d + 2 - 4 * odd
    second = d - 2 + 4 * odd
    has_across = (across >= 0) & (across < width)
    has_beyond = (beyond >= 0) & (beyond < width)

    even = lax.rem(g, 2) == 0
    down_two = even & (g > 1)
    down_one = down_two | (g == top)
    copies = (lax.rem(g, 2) == 1) & (g < top)
    twice = (lax.rem(g, 2) == 0) & (g + 1 < top)
    stages = jnp.where(twice, 2, 1)
    last = stages * sweeps

    loads = [
        pltpu.make_async_copy(nbr_hbm, nbr, load_sem.at[0]),
        pltpu.make_async_copy(face_hbm, face, load_sem.at[1]),
        pltpu.make_async_copy(cell_hbm, cell, load_sem.at[2]),
        pltpu.make_async_copy(volume_hbm, volume, load_sem.at[3]),
        pltpu.make_async_copy(jac_hbm.at[0], jac.at[0], load_sem.at[4]),
        pltpu.make_async_copy(terminal_hbm, terminal, load_sem.at[5]),
        pltpu.make_async_copy(source_hbm, source.at[0], load_sem.at[6]),
        pltpu.make_async_copy(shape_hbm, shape, load_sem.at[7]),
    ]
    for load in loads:
        load.start()

    @pl.when(jnp.logical_not(has_across))
    def _():
        from_across[...] = jnp.zeros_like(from_across)

    barrier = pltpu.get_barrier_semaphore()
    for other in range(groups):
        @pl.when(g != other)
        def _():
            pl.semaphore_signal(barrier, inc=1, device_id={"tm": other})

    up_two = even & (g + 2 < groups)
    up_one = (jnp.logical_not(even) & (g + 1 < groups)) | (g + 1 == top)

    def greet(side):
        pl.semaphore_signal(barrier, inc=1, device_id={"space": side})
        for shift, linked in ((-2, down_two), (-1, down_one), (1, up_one), (2, up_two)):
            @pl.when(linked)
            def _():
                pl.semaphore_signal(barrier, inc=1, device_id={"tm": g + shift, "space": side})

    for shift in (1, 2):
        @pl.when(d > shift - 1)
        def _():
            greet(d - shift)

        @pl.when(d < width - shift)
        def _():
            greet(d + shift)

    sides = sum(jnp.where(d > i - 1, 1, 0) + jnp.where(d < width - i, 1, 0) for i in (1, 2))
    slabs = 1 + sum(jnp.where(linked, 1, 0) for linked in (down_two, down_one, up_one, up_two))
    expected = groups - 1 + sides * slabs

    def jac_copy(to):
        return pltpu.make_async_remote_copy(
            src_ref=jac_hbm.at[0], dst_ref=jac.at[1], send_sem=copy_send.at[0],
            recv_sem=copy_recv.at[0], device_id={"tm": to},
        )

    def source_copy(n, to):
        return pltpu.make_async_remote_copy(
            src_ref=source_hbm.at[n], dst_ref=source.at[1, n], send_sem=copy_send.at[1 + n],
            recv_sem=copy_recv.at[1 + n], device_id={"tm": to},
        )

    @pl.when(copies)
    def _():
        pl.semaphore_wait(barrier, expected)
        jac_copy(g - 1).start()
        for n in reversed(range(steps)):
            source_copy(n, g - 1).start()

    halo_terms[...] = jnp.zeros_like(halo_terms)
    edge_terms[...] = jnp.zeros_like(edge_terms)
    edge_halo[...] = jnp.zeros_like(edge_halo)
    lane = lax.broadcasted_iota(jnp.int32, (1, nb), 1)
    for i in range(2):
        for s in range(count):
            row = i * count + s
            block = jnp.where(odd == i, send_blocks[0, 1, s], send_blocks[0, 0, s])
            select[pl.ds(row, 1), :] = jnp.where(lane == block, 1.0, 0.0)
    chosen_low = select[...].astype(jnp.bfloat16)
    select_terms[:, :nb] = chosen_low
    select_terms[:, nb:] = chosen_low
    chosen = select[count:edges, :]
    chosen_low = chosen.astype(jnp.bfloat16)

    loads[0].wait()
    listed = nbr[...].astype(jnp.float32)
    listed = jnp.concatenate([listed, jnp.zeros((nb - nei, nb), jnp.float32)], axis=0).T
    wide = lax.broadcasted_iota(jnp.int32, (nb, nb), 1).astype(jnp.float32)
    swap = ((1 - odd) * count).astype(jnp.float32)
    for k in range(nei):
        column = jnp.broadcast_to(listed[:, k : k + 1], (nb, nb))
        pick = jnp.where(column == wide, 1.0, 0.0).astype(jnp.bfloat16)
        near_pick[pl.ds(k * nb, nb), :nb] = pick
        near_pick[pl.ds(k * nb, nb), nb:] = pick
        shifted = column - nb
        inside = (shifted >= 0) & (shifted < edges)
        shifted = shifted + swap * jnp.where(shifted < count, 1.0, -1.0)
        hit = (shifted == wide) | (shifted + edges == wide)
        pick = jnp.where(hit & inside, 1.0, 0.0).astype(jnp.bfloat16)
        far_pick[pl.ds(k * nb, nb), :] = pick
        own_fixed[k] = matmul(chosen_low, pick)

    for load in loads[1:5]:
        load.wait()
    alive = live_count[0]
    row_id = lax.broadcasted_iota(jnp.int32, (TILE, cells), 0)
    lane_id = lax.broadcasted_iota(jnp.int32, (TILE, cells), 1)

    def live_of(t):
        return jnp.where(row_id + t * TILE < alive, 1.0, 0.0)

    def prepare(t, store):
        r = rows_at(t * TILE)
        live = live_of(t)
        mass = INVERSE_STEP * volume[r, :]
        along = cell[r, :]
        base = mass + 2.0 * along
        for k in range(nei):
            base = base + face[k, r, :]
        if store == 0:
            cell_left[r, :] = jnp.where(lane_id == 0, 0.0, along)
            cell_right[r, :] = jnp.where(lane_id == cells - 1, 0.0, along)
        for j in range(comp):
            c = live / (base + jac[store, j, j, r, :])
            rate[store, j, r, :] = c
            drift = c * mass
            rate_mass[store, j, r, :] = drift
            for i in range(comp):
                entry = -c * jac[store, i, j, r, :]
                jac[store, i, j, r, :] = entry + (live - drift) if i == j else entry
            if store == 0:
                weighted[j, r, :] = jnp.zeros((TILE, cells), jnp.float32)

    def fixed_copy():
        return pltpu.make_async_remote_copy(
            src_ref=own_fixed, dst_ref=their_fixed, send_sem=coef_send.at[0],
            recv_sem=coef_recv.at[0], device_id={"space": across},
        )

    def rate_copy(store):
        return pltpu.make_async_remote_copy(
            src_ref=own_rate.at[store], dst_ref=their_rate.at[store], send_sem=coef_send.at[1 + store],
            recv_sem=coef_recv.at[1 + store], device_id={"space": across},
        )

    for t in range(tiles):
        prepare(t, 0)
    for k in range(nei):
        own_fixed[nei + k] = matmul(chosen, face[k], HIGHEST)
    for j in range(comp):
        own_rate[0, j] = matmul(chosen, rate[0, j], HIGHEST)

    for load in loads[5:]:
        load.wait()

    @pl.when(jnp.logical_not(copies))
    def _():
        pl.semaphore_wait(barrier, expected)

    def lanes(j):
        return slice(j * cells, (j + 1) * cells)

    def put_terms(ref, t, j, x):
        high, low = split(x)
        ref[rows_at(t * TILE), lanes(j)] = high
        ref[rows_at(nb + t * TILE), lanes(j)] = low

    def put_edges(ref, side, j, x):
        high, low = split(x)
        ref[side * count : (side + 1) * count, lanes(j)] = high
        ref[edges + side * count : edges + (side + 1) * count, lanes(j)] = low

    def state_copy(way, to):
        return pltpu.make_async_remote_copy(
            src_ref=field, dst_ref=field, send_sem=state_send.at[way], recv_sem=state_recv,
            device_id={"tm": to},
        )

    def partner_copy(slot):
        return pltpu.make_async_remote_copy(
            src_ref=edge_out.at[slot + 1, 0], dst_ref=from_partner.at[slot],
            send_sem=partner_send.at[slot], recv_sem=partner_recv.at[slot],
            device_id={"space": partner},
        )

    def second_copy(slot, to):
        return pltpu.make_async_remote_copy(
            src_ref=edge_out.at[slot + 1, 0], dst_ref=from_second.at[slot + 1],
            send_sem=second_send.at[slot + 1], recv_sem=second_recv.at[slot + 1],
            device_id={"space": to},
        )

    def across_copy(slot):
        return pltpu.make_async_remote_copy(
            src_ref=part_out.at[slot], dst_ref=from_across.at[slot],
            send_sem=across_send.at[slot], recv_sem=across_recv.at[slot],
            device_id={"space": across},
        )

    def first_copies(slot, way, to):
        kinds = ((0, partner, from_partner.at[0], partner_recv.at[0]),
                 (1, across, from_across.at[0], across_recv.at[0]),
                 (0, beyond, from_second.at[1], second_recv.at[1]))
        return [
            pltpu.make_async_remote_copy(
                src_ref=edge_out.at[slot + 1, side], dst_ref=ref,
                send_sem=first_send.at[way, i], recv_sem=recv,
                device_id={"tm": to, "space": place},
            )
            for i, (side, place, ref, recv) in enumerate(kinds)
        ]

    def first_send_all(slot, way, to):
        near_one, across_one, second_one = first_copies(slot, way, to)

        @pl.when(has_across)
        def _():
            across_one.start()

        @pl.when(has_beyond)
        def _():
            second_one.start()

        near_one.start()

    def first_drain(slot, way, to):
        near_one, across_one, second_one = first_copies(slot, way, to)

        @pl.when(has_across)
        def _():
            across_one.wait_send()

        @pl.when(has_beyond)
        def _():
            second_one.wait_send()

        near_one.wait_send()

    def choose(slot):
        values = matmul(select_terms[...], field_terms[...])
        for side in range(2):
            for j in range(comp):
                edge_out[slot + 1, side, j] = values[side * count : (side + 1) * count, lanes(j)]

    @pl.when(g == top)
    def _():
        for t in range(tiles):
            r = rows_at(t * TILE)
            for j in range(comp):
                x = live_of(t) * terminal[j, r, :]
                field[j, r, :] = x
                put_terms(field_terms, t, j, x)
        choose(-1)
        first_send_all(-1, 0, g)

    @pl.when(has_across)
    def _():
        fixed_copy().start()
        rate_copy(0).start()

    @pl.when(twice)
    def _():
        jac_copy(g).wait_recv()
        for t in range(tiles):
            prepare(t, 1)
        for j in range(comp):
            own_rate[1, j] = matmul(chosen, rate[1, j], HIGHEST)

        @pl.when(has_across)
        def _():
            rate_copy(1).start()

    @pl.when(g < top)
    def _():
        state_copy(0, g).wait_recv()
        for t in range(tiles):
            for j in range(comp):
                put_terms(field_terms, t, j, field[j, rows_at(t * TILE), :])

    def sweep(m):
        store = jnp.where(twice & (m < sweeps), 1, 0)
        choose(m)

        @pl.when(m > 0)
        def _():
            partner_copy(m).start()

            @pl.when(has_beyond & (m < last - 1))
            def _():
                second_copy(m, beyond).start()

        near[...] = matmul(near_pick[...], field_terms[...])

        for t in range(tiles):
            r = rows_at(t * TILE)
            x = [field[i, r, :] for i in range(comp)]
            left = cell_left[r, :]
            right = cell_right[r, :]
            for j in range(comp):
                value = left * pltpu.roll(x[j], 1, 1) + right * pltpu.roll(x[j], cells - 1, 1)
                for k in range(nei):
                    q = rows_at(k * nb + t * TILE)
                    value = value + face[k, r, :] * near[q, lanes(j)]
                value = rhs[j, r, :] + rate[store, j, r, :] * value
                for i in range(comp):
                    value = value + jac[store, i, j, r, :] * x[i]
                part[j, r, :] = value
                put_terms(part_terms, t, j, value)

        @pl.when(has_across & (m < last - 1))
        def _():
            ahead = matmul(select_terms[count:edges, :], part_terms[...])
            for j in range(comp):
                part_out[m + 1, j] = ahead[:, lanes(j)]
            across_copy(m + 1).start()

        @pl.when(has_across & (m == 1))
        def _():
            fixed_copy().wait_recv()
            rate_copy(0).wait_recv()
            for k in range(nei):
                their_pick[k * count : (k + 1) * count, :] = their_fixed[k].astype(jnp.bfloat16)

            @pl.when(twice)
            def _():
                rate_copy(1).wait_recv()

        @pl.when(has_across & (m > 0))
        def _():
            kept = jnp.where(twice & (m <= sweeps), 1, 0)
            second_copy(m - 1, second).wait_recv()
            for side in range(2):
                for j in range(comp):
                    put_edges(edge_terms, side, j, from_second[m, j] if side == 0 else edge_out[m, 1, j])
            arrived = matmul(their_pick[...], edge_terms[...])
            for j in range(comp):
                value = None
                for k in range(nei):
                    term = their_fixed[nei + k] * arrived[k * count : (k + 1) * count, lanes(j)]
                    value = term if value is None else value + term
                edge_halo[j] = their_rate[kept, j] * value

        partner_copy(m).wait_recv()
        for j in range(comp):
            put_edges(halo_terms, 0, j, from_partner[m, j])

        @pl.when(has_across)
        def _():
            across_copy(m).wait_recv()

        for j in range(comp):
            put_edges(halo_terms, 1, j, from_across[m, j] + edge_halo[j])

        far[...] = matmul(far_pick[...], halo_terms[...])

        for t in range(tiles):
            r = rows_at(t * TILE)
            for j in range(comp):
                value = None
                for k in range(nei):
                    q = rows_at(k * nb + t * TILE)
                    term = face[k, r, :] * far[q, lanes(j)]
                    value = term if value is None else value + term
                value = part[j, r, :] + rate[store, j, r, :] * value
                field[j, r, :] = value
                put_terms(field_terms, t, j, value)

    def level_copy(n):
        return pltpu.make_async_copy(levels.at[n], adjoint_hbm.at[n], store_sem.at[n])

    def level(step, _):
        copied = twice & (step < steps)
        store = jnp.where(copied, 1, 0)
        n = steps - 1 - lax.rem(step, steps)

        @pl.when(copied)
        def _():
            source_copy(n, g).wait_recv()

        for t in range(tiles):
            r = rows_at(t * TILE)
            for j in range(comp):
                rhs[j, r, :] = (
                    rate[store, j, r, :] * source[store, n, j, r, :] + rate_mass[store, j, r, :] * field[j, r, :]
                )

        def one(it, _):
            sweep(step * ITERS + it)
            return 0

        lax.fori_loop(0, ITERS, one, 0)

        @pl.when((step == stages * steps - 1) & down_one)
        def _():
            @pl.when(down_two)
            def _():
                state_copy(0, g - 2).start()

            choose(last)

            @pl.when(down_two)
            def _():
                first_send_all(last, 0, g - 2)

            state_copy(1, g - 1).start()
            first_send_all(last, 1, g - 1)

        @pl.when(jnp.logical_not(copied))
        def _():
            weight = weights[n]
            for t in range(tiles):
                r = rows_at(t * TILE)
                for j in range(comp):
                    x = field[j, r, :]
                    levels[n, j, r, :] = x
                    weighted[j, r, :] = weighted[j, r, :] + weight * x
            level_copy(n).start()

        return 0

    def level_if(step, _):
        @pl.when(step < stages * steps)
        def _():
            level(step, 0)

        return 0

    lax.fori_loop(0, 2 * steps, level_if, 0)

    summed = jnp.zeros((nb, cells), jnp.float32)
    for j in range(comp):
        summed = summed + weighted[j] * shape[j]

    mine = lax.dot_general(
        jnp.ones((8, cells), jnp.float32),
        summed,
        (((1,), (1,)), ((), ())),
        precision=lax.Precision.HIGHEST,
        preferred_element_type=jnp.float32,
    )

    def acc_copy(to):
        return pltpu.make_async_remote_copy(
            src_ref=acc_out, dst_ref=acc_in, send_sem=acc_send, recv_sem=acc_recv,
            device_id={"tm": to},
        )

    def total_copy(to):
        return pltpu.make_async_remote_copy(
            src_ref=acc_out, dst_ref=total, send_sem=total_send.at[to], recv_sem=total_recv,
            device_id={"tm": to},
        )

    @pl.when(g == top)
    def _():
        acc_out[...] = mine

    @pl.when(g < top)
    def _():
        acc_copy(g).wait_recv()
        acc_out[...] = mine + acc_in[...]

    @pl.when(g > 0)
    def _():
        acc_copy(g - 1).start()
        total_copy(g).wait_recv()
        sens_ref[...] = total[0:1, :]

    @pl.when(g == 0)
    def _():
        for other in range(1, groups):
            total_copy(other).start()
        sens_ref[...] = acc_out[0:1, :]
        for other in range(1, groups):
            total_copy(other).wait_send()

    @pl.when(g > 0)
    def _():
        acc_copy(g - 1).wait_send()

    @pl.when(copies)
    def _():
        jac_copy(g - 1).wait_send()
        for n in range(steps):
            source_copy(n, g - 1).wait_send()

    @pl.when(has_across)
    def _():
        fixed_copy().wait_send()
        rate_copy(0).wait_send()

        @pl.when(twice)
        def _():
            rate_copy(1).wait_send()

    @pl.when(g == top)
    def _():
        first_drain(-1, 0, g)

    @pl.when(down_two)
    def _():
        state_copy(0, g - 2).wait_send()
        first_drain(last, 0, g - 2)

    @pl.when(down_one)
    def _():
        state_copy(1, g - 1).wait_send()
        first_drain(last, 1, g - 1)

    def drain(slot, _):
        @pl.when(slot < last)
        def _():
            partner_copy(slot).wait_send()

        @pl.when(has_beyond & (slot < last - 1))
        def _():
            second_copy(slot, beyond).wait_send()

        @pl.when(has_across & (slot < last))
        def _():
            across_copy(slot).wait_send()

        return 0

    lax.fori_loop(1, 2 * sweeps, drain, 0)
    for n in range(steps):
        level_copy(n).wait()


def per_device(groups, width, *args):
    (source, terminal, jacobian, face_coef, cell_coef, neighbours, send_blocks,
     live_count, volume, shape_field, weights) = args
    steps, nb, comp, cells = source.shape
    nei = face_coef.shape[1]
    count = send_blocks.shape[2]
    edges = 2 * count
    slots = 2 * steps * ITERS
    f32 = jnp.float32
    bf16 = jnp.bfloat16
    hbm = pl.BlockSpec(memory_space=pltpu.MemorySpace.HBM)
    smem = pl.BlockSpec(memory_space=pltpu.SMEM)
    vmem = pltpu.VMEM
    dma = pltpu.SemaphoreType.DMA
    block = (comp, nb, cells)
    flat = comp * cells
    edge = (comp, count, cells)
    adjoint, sens = pl.pallas_call(
        functools.partial(kernel, groups, width),
        out_shape=(
            jax.ShapeDtypeStruct((steps, comp, nb, cells), f32),
            jax.ShapeDtypeStruct((1, nb), f32),
        ),
        in_specs=[hbm, hbm, hbm, hbm, hbm, hbm, smem, smem, hbm, hbm, smem],
        out_specs=(hbm, pl.BlockSpec(memory_space=pltpu.VMEM)),
        scratch_shapes=[
            vmem((2, steps, comp, nb, cells), f32),
            vmem(block, f32),
            vmem((2, comp, comp, nb, cells), f32),
            vmem((nei, nb, cells), f32),
            vmem((nb, cells), f32),
            vmem((nei, nb), jnp.int32),
            vmem((nb, cells), f32),
            vmem(block, f32),
            vmem(block, f32),
            vmem(block, f32),
            vmem((2,) + block, f32),
            vmem((2,) + block, f32),
            vmem((nb, cells), f32),
            vmem((nb, cells), f32),
            vmem(block, f32),
            vmem((steps, comp, nb, cells), f32),
            vmem(block, f32),
            vmem((nei * nb, 2 * nb), bf16),
            vmem((nei * nb, nb), bf16),
            vmem((2 * nb, flat), bf16),
            vmem((2 * nb, flat), bf16),
            vmem((nb, flat), bf16),
            vmem((nb, flat), bf16),
            vmem((nei * nb, flat), f32),
            vmem((nei * nb, flat), f32),
            vmem((edges, nb), f32),
            vmem((edges, 2 * nb), bf16),
            vmem((2 * nei, count, cells), f32),
            vmem((2,) + edge, f32),
            vmem((2 * nei, count, cells), f32),
            vmem((2,) + edge, f32),
            vmem((nei * count, nb), bf16),
            vmem(edge, f32),
            vmem((slots + 1,) + edge, f32),
            vmem((slots + 1,) + edge, f32),
            vmem((slots + 1,) + edge, f32),
            vmem((slots + 2, 2) + edge, f32),
            vmem((slots + 1,) + edge, f32),
            vmem((8, nb), f32),
            vmem((8, nb), f32),
            vmem((8, nb), f32),
            dma((8,)),
            dma((steps,)),
            dma((1 + steps,)),
            dma((1 + steps,)),
            dma((3,)),
            dma((3,)),
            dma((slots + 1,)),
            dma((slots + 1,)),
            dma((slots + 1,)),
            dma((slots + 1,)),
            dma((slots + 1,)),
            dma((slots + 1,)),
            dma((2, 3)),
            dma((2,)),
            dma,
            dma,
            dma,
            dma((groups,)),
            dma,
        ],
        compiler_params=pltpu.CompilerParams(collective_id=0, has_side_effects=True),
    )(
        source.transpose(0, 2, 1, 3),
        terminal.transpose(1, 0, 2),
        jacobian.transpose(0, 2, 3, 1, 4),
        face_coef.transpose(1, 0, 2),
        cell_coef,
        neighbours.T,
        send_blocks,
        live_count,
        volume,
        shape_field.transpose(1, 0, 2),
        weights,
    )
    return adjoint.transpose(0, 2, 1, 3), sens.reshape(nb)


def solution(mesh):
    sizes = dict(mesh.shape)
    return jax.shard_map(
        functools.partial(per_device, sizes["tm"], sizes["space"]),
        mesh=mesh,
        in_specs=(
            P("tm", "space", None, None),
            P("space", None, None),
            P("tm", "space", None, None, None),
            P("space", None, None),
            P("space", None),
            P("space", None),
            P("space", None, None),
            P("space"),
            P("space", None),
            P("space", None, None),
            P("tm"),
        ),
        out_specs=(P("tm", "space", None, None), P("space")),
        check_vma=False,
    )
```

```python
import functools

import jax
import jax.numpy as jnp
from jax import lax
from jax.experimental import pallas as pl
from jax.experimental.pallas import tpu as pltpu
from jax.sharding import PartitionSpec as P

ITERS = 3
INVERSE_STEP = 6.0
TILE = 16


def rows_at(start):
    return pl.ds(start if isinstance(start, int) else pl.multiple_of(start, TILE), TILE)


def split(x):
    high = x.astype(jnp.bfloat16)
    return high, (x - high.astype(jnp.float32)).astype(jnp.bfloat16)


def matmul(a, b):
    return jnp.dot(a, b, preferred_element_type=jnp.float32)


def kernel(
    groups,
    width,
    source_hbm,
    terminal_hbm,
    jac_hbm,
    face_hbm,
    cell_hbm,
    nbr_hbm,
    send_blocks,
    live_count,
    volume_hbm,
    shape_hbm,
    weights,
    adjoint_hbm,
    sens_ref,
    source,
    terminal,
    jac,
    face,
    cell,
    nbr,
    volume,
    shape,
    field,
    part,
    rate,
    rate_mass,
    cell_left,
    cell_right,
    rhs,
    levels,
    weighted,
    near_pick,
    far_pick,
    field_terms,
    halo_terms,
    edge_terms,
    near,
    far,
    select,
    own_fixed,
    own_rate,
    their_fixed,
    their_rate,
    their_pick,
    edge_halo,
    from_partner,
    from_across,
    from_second,
    edge_out,
    part_out,
    acc_in,
    acc_out,
    total,
    load_sem,
    store_sem,
    copy_send,
    copy_recv,
    coef_send,
    coef_recv,
    partner_send,
    partner_recv,
    across_send,
    across_recv,
    second_send,
    second_recv,
    first_send,
    state_send,
    state_recv,
    acc_send,
    acc_recv,
    total_send,
    total_recv,
):
    g = lax.axis_index("tm")
    d = lax.axis_index("space")
    _, steps, comp, nb, cells = source.shape
    nei = face.shape[0]
    count = edge_out.shape[3]
    sweeps = steps * ITERS
    tiles = nb // TILE
    edges = 2 * count
    top = groups - 1

    odd = lax.rem(d, 2)
    partner = d + 1 - 2 * odd
    across = d - 1 + 2 * odd
    beyond = d + 2 - 4 * odd
    second = d - 2 + 4 * odd
    has_across = (across >= 0) & (across < width)
    has_beyond = (beyond >= 0) & (beyond < width)

    even = lax.rem(g, 2) == 0
    down_two = even & (g > 1)
    down_one = down_two | (g == top)
    copies = (lax.rem(g, 2) == 1) & (g < top)
    twice = (lax.rem(g, 2) == 0) & (g + 1 < top)
    stages = jnp.where(twice, 2, 1)
    last = stages * sweeps

    loads = [
        pltpu.make_async_copy(nbr_hbm, nbr, load_sem.at[0]),
        pltpu.make_async_copy(face_hbm, face, load_sem.at[1]),
        pltpu.make_async_copy(cell_hbm, cell, load_sem.at[2]),
        pltpu.make_async_copy(volume_hbm, volume, load_sem.at[3]),
        pltpu.make_async_copy(jac_hbm.at[0], jac.at[0], load_sem.at[4]),
        pltpu.make_async_copy(terminal_hbm, terminal, load_sem.at[5]),
        pltpu.make_async_copy(source_hbm, source.at[0], load_sem.at[6]),
        pltpu.make_async_copy(shape_hbm, shape, load_sem.at[7]),
    ]
    for load in loads:
        load.start()

    @pl.when(jnp.logical_not(has_across))
    def _():
        from_across[...] = jnp.zeros_like(from_across)

    barrier = pltpu.get_barrier_semaphore()
    for other in range(groups):
        @pl.when(g != other)
        def _():
            pl.semaphore_signal(barrier, inc=1, device_id={"tm": other})

    up_two = even & (g + 2 < groups)
    up_one = (jnp.logical_not(even) & (g + 1 < groups)) | (g + 1 == top)

    def greet(side):
        pl.semaphore_signal(barrier, inc=1, device_id={"space": side})
        for shift, linked in ((-2, down_two), (-1, down_one), (1, up_one), (2, up_two)):
            @pl.when(linked)
            def _():
                pl.semaphore_signal(barrier, inc=1, device_id={"tm": g + shift, "space": side})

    for shift in (1, 2):
        @pl.when(d > shift - 1)
        def _():
            greet(d - shift)

        @pl.when(d < width - shift)
        def _():
            greet(d + shift)

    sides = sum(jnp.where(d > i - 1, 1, 0) + jnp.where(d < width - i, 1, 0) for i in (1, 2))
    slabs = 1 + sum(jnp.where(linked, 1, 0) for linked in (down_two, down_one, up_one, up_two))
    expected = groups - 1 + sides * slabs

    def jac_copy(to):
        return pltpu.make_async_remote_copy(
            src_ref=jac_hbm.at[0], dst_ref=jac.at[1], send_sem=copy_send.at[0],
            recv_sem=copy_recv.at[0], device_id={"tm": to},
        )

    def source_copy(n, to):
        return pltpu.make_async_remote_copy(
            src_ref=source_hbm.at[n], dst_ref=source.at[1, n], send_sem=copy_send.at[1 + n],
            recv_sem=copy_recv.at[1 + n], device_id={"tm": to},
        )

    @pl.when(copies)
    def _():
        pl.semaphore_wait(barrier, expected)
        jac_copy(g - 1).start()
        for n in reversed(range(steps)):
            source_copy(n, g - 1).start()

    def block_of(side, s):
        return jnp.where(odd == side, send_blocks[0, 1, s], send_blocks[0, 0, s])

    halo_terms[...] = jnp.zeros_like(halo_terms)
    edge_terms[...] = jnp.zeros_like(edge_terms)
    edge_halo[...] = jnp.zeros_like(edge_halo)
    lane = lax.broadcasted_iota(jnp.int32, (1, nb), 1)
    for s in range(count):
        select[pl.ds(s, 1), :] = jnp.where(lane == block_of(1, s), 1.0, 0.0)
    chosen = select[...].astype(jnp.bfloat16)

    loads[0].wait()
    listed = nbr[...].astype(jnp.float32)
    listed = jnp.concatenate([listed, jnp.zeros((nb - nei, nb), jnp.float32)], axis=0).T
    wide = lax.broadcasted_iota(jnp.int32, (nb, nb), 1).astype(jnp.float32)
    swap = ((1 - odd) * count).astype(jnp.float32)
    for k in range(nei):
        column = jnp.broadcast_to(listed[:, k : k + 1], (nb, nb))
        pick = jnp.where(column == wide, 1.0, 0.0).astype(jnp.bfloat16)
        near_pick[pl.ds(k * nb, nb), :nb] = pick
        near_pick[pl.ds(k * nb, nb), nb:] = pick
        shifted = column - nb
        inside = (shifted >= 0) & (shifted < edges)
        shifted = shifted + swap * jnp.where(shifted < count, 1.0, -1.0)
        hit = (shifted == wide) | (shifted + edges == wide)
        pick = jnp.where(hit & inside, 1.0, 0.0).astype(jnp.bfloat16)
        far_pick[pl.ds(k * nb, nb), :] = pick
        own_fixed[k] = matmul(chosen, pick)

    for load in loads[1:5]:
        load.wait()
    alive = live_count[0]
    row_id = lax.broadcasted_iota(jnp.int32, (TILE, cells), 0)
    lane_id = lax.broadcasted_iota(jnp.int32, (TILE, cells), 1)

    def live_of(t):
        return jnp.where(row_id + t * TILE < alive, 1.0, 0.0)

    def prepare(t, store):
        r = rows_at(t * TILE)
        live = live_of(t)
        mass = INVERSE_STEP * volume[r, :]
        along = cell[r, :]
        base = mass + 2.0 * along
        for k in range(nei):
            base = base + face[k, r, :]
        if store == 0:
            cell_left[r, :] = jnp.where(lane_id == 0, 0.0, along)
            cell_right[r, :] = jnp.where(lane_id == cells - 1, 0.0, along)
        for j in range(comp):
            c = live / (base + jac[store, j, j, r, :])
            rate[store, j, r, :] = c
            drift = c * mass
            rate_mass[store, j, r, :] = drift
            for i in range(comp):
                entry = -c * jac[store, i, j, r, :]
                jac[store, i, j, r, :] = entry + (live - drift) if i == j else entry
            if store == 0:
                weighted[j, r, :] = jnp.zeros((TILE, cells), jnp.float32)

    def fixed_copy():
        return pltpu.make_async_remote_copy(
            src_ref=own_fixed, dst_ref=their_fixed, send_sem=coef_send.at[0],
            recv_sem=coef_recv.at[0], device_id={"space": across},
        )

    def rate_copy(store):
        return pltpu.make_async_remote_copy(
            src_ref=own_rate.at[store], dst_ref=their_rate.at[store], send_sem=coef_send.at[1 + store],
            recv_sem=coef_recv.at[1 + store], device_id={"space": across},
        )

    for t in range(tiles):
        prepare(t, 0)
    for s in range(count):
        block = pl.ds(block_of(1, s), 1)
        for k in range(nei):
            own_fixed[nei + k, pl.ds(s, 1), :] = face[k, block, :]
        for j in range(comp):
            own_rate[0, j, pl.ds(s, 1), :] = rate[0, j, block, :]

    for load in loads[5:]:
        load.wait()

    @pl.when(jnp.logical_not(copies))
    def _():
        pl.semaphore_wait(barrier, expected)

    def lanes(j):
        return slice(j * cells, (j + 1) * cells)

    def put_terms(ref, t, j, x):
        high, low = split(x)
        ref[rows_at(t * TILE), lanes(j)] = high
        ref[rows_at(nb + t * TILE), lanes(j)] = low

    def put_edges(ref, side, j, x):
        high, low = split(x)
        ref[side * count : (side + 1) * count, lanes(j)] = high
        ref[edges + side * count : edges + (side + 1) * count, lanes(j)] = low

    def state_copy(way, to):
        return pltpu.make_async_remote_copy(
            src_ref=field, dst_ref=field, send_sem=state_send.at[way], recv_sem=state_recv,
            device_id={"tm": to},
        )

    def partner_copy(slot):
        return pltpu.make_async_remote_copy(
            src_ref=edge_out.at[slot + 1, 0], dst_ref=from_partner.at[slot],
            send_sem=partner_send.at[slot], recv_sem=partner_recv.at[slot],
            device_id={"space": partner},
        )

    def second_copy(slot, to):
        return pltpu.make_async_remote_copy(
            src_ref=edge_out.at[slot + 1, 0], dst_ref=from_second.at[slot + 1],
            send_sem=second_send.at[slot + 1], recv_sem=second_recv.at[slot + 1],
            device_id={"space": to},
        )

    def across_copy(slot):
        return pltpu.make_async_remote_copy(
            src_ref=part_out.at[slot], dst_ref=from_across.at[slot],
            send_sem=across_send.at[slot], recv_sem=across_recv.at[slot],
            device_id={"space": across},
        )

    def first_copies(slot, way, to):
        kinds = ((0, partner, from_partner.at[0], partner_recv.at[0]),
                 (1, across, from_across.at[0], across_recv.at[0]),
                 (0, beyond, from_second.at[1], second_recv.at[1]))
        return [
            pltpu.make_async_remote_copy(
                src_ref=edge_out.at[slot + 1, side], dst_ref=ref,
                send_sem=first_send.at[way, i], recv_sem=recv,
                device_id={"tm": to, "space": place},
            )
            for i, (side, place, ref, recv) in enumerate(kinds)
        ]

    def first_send_all(slot, way, to):
        near_one, across_one, second_one = first_copies(slot, way, to)

        @pl.when(has_across)
        def _():
            across_one.start()

        @pl.when(has_beyond)
        def _():
            second_one.start()

        near_one.start()

    def first_drain(slot, way, to):
        near_one, across_one, second_one = first_copies(slot, way, to)

        @pl.when(has_across)
        def _():
            across_one.wait_send()

        @pl.when(has_beyond)
        def _():
            second_one.wait_send()

        near_one.wait_send()

    def choose(slot, side):
        for s in range(count):
            for j in range(comp):
                edge_out[slot + 1, side, j, pl.ds(s, 1), :] = field[j, pl.ds(block_of(side, s), 1), :]

    @pl.when(g == top)
    def _():
        for t in range(tiles):
            r = rows_at(t * TILE)
            for j in range(comp):
                x = live_of(t) * terminal[j, r, :]
                field[j, r, :] = x
                put_terms(field_terms, t, j, x)
        for side in range(2):
            choose(-1, side)
        first_send_all(-1, 0, g)

    @pl.when(has_across)
    def _():
        fixed_copy().start()
        rate_copy(0).start()

    @pl.when(twice)
    def _():
        jac_copy(g).wait_recv()
        for t in range(tiles):
            prepare(t, 1)
        for s in range(count):
            for j in range(comp):
                own_rate[1, j, pl.ds(s, 1), :] = rate[1, j, pl.ds(block_of(1, s), 1), :]

        @pl.when(has_across)
        def _():
            rate_copy(1).start()

    @pl.when(g < top)
    def _():
        state_copy(0, g).wait_recv()
        for t in range(tiles):
            for j in range(comp):
                put_terms(field_terms, t, j, field[j, rows_at(t * TILE), :])

    def sweep(m):
        store = jnp.where(twice & (m < sweeps), 1, 0)
        choose(m, 0)

        @pl.when(m > 0)
        def _():
            partner_copy(m).start()

            @pl.when(has_beyond & (m < last - 1))
            def _():
                second_copy(m, beyond).start()

        choose(m, 1)
        near[...] = matmul(near_pick[...], field_terms[...])

        for t in range(tiles):
            r = rows_at(t * TILE)
            x = [field[i, r, :] for i in range(comp)]
            left = cell_left[r, :]
            right = cell_right[r, :]
            for j in range(comp):
                value = left * pltpu.roll(x[j], 1, 1) + right * pltpu.roll(x[j], cells - 1, 1)
                for k in range(nei):
                    q = rows_at(k * nb + t * TILE)
                    value = value + face[k, r, :] * near[q, lanes(j)]
                value = rhs[j, r, :] + rate[store, j, r, :] * value
                for i in range(comp):
                    value = value + jac[store, i, j, r, :] * x[i]
                part[j, r, :] = value

        @pl.when(has_across & (m < last - 1))
        def _():
            for s in range(count):
                for j in range(comp):
                    part_out[m + 1, j, pl.ds(s, 1), :] = part[j, pl.ds(block_of(1, s), 1), :]
            across_copy(m + 1).start()

        @pl.when(has_across & (m == 1))
        def _():
            fixed_copy().wait_recv()
            rate_copy(0).wait_recv()
            for k in range(nei):
                their_pick[k * count : (k + 1) * count, :] = their_fixed[k].astype(jnp.bfloat16)

            @pl.when(twice)
            def _():
                rate_copy(1).wait_recv()

        @pl.when(has_across & (m > 0))
        def _():
            kept = jnp.where(twice & (m <= sweeps), 1, 0)
            second_copy(m - 1, second).wait_recv()
            for side in range(2):
                for j in range(comp):
                    put_edges(edge_terms, side, j, from_second[m, j] if side == 0 else edge_out[m, 1, j])
            arrived = matmul(their_pick[...], edge_terms[...])
            for j in range(comp):
                value = None
                for k in range(nei):
                    term = their_fixed[nei + k] * arrived[k * count : (k + 1) * count, lanes(j)]
                    value = term if value is None else value + term
                edge_halo[j] = their_rate[kept, j] * value

        partner_copy(m).wait_recv()
        for j in range(comp):
            put_edges(halo_terms, 0, j, from_partner[m, j])

        @pl.when(has_across)
        def _():
            across_copy(m).wait_recv()

        for j in range(comp):
            put_edges(halo_terms, 1, j, from_across[m, j] + edge_halo[j])

        far[...] = matmul(far_pick[...], halo_terms[...])

        for t in range(tiles):
            r = rows_at(t * TILE)
            for j in range(comp):
                value = None
                for k in range(nei):
                    q = rows_at(k * nb + t * TILE)
                    term = face[k, r, :] * far[q, lanes(j)]
                    value = term if value is None else value + term
                value = part[j, r, :] + rate[store, j, r, :] * value
                field[j, r, :] = value
                put_terms(field_terms, t, j, value)

    def level_copy(n):
        return pltpu.make_async_copy(levels.at[n], adjoint_hbm.at[n], store_sem.at[n])

    def level(step, _):
        copied = twice & (step < steps)
        store = jnp.where(copied, 1, 0)
        n = steps - 1 - lax.rem(step, steps)

        @pl.when(copied)
        def _():
            source_copy(n, g).wait_recv()

        for t in range(tiles):
            r = rows_at(t * TILE)
            for j in range(comp):
                rhs[j, r, :] = (
                    rate[store, j, r, :] * source[store, n, j, r, :] + rate_mass[store, j, r, :] * field[j, r, :]
                )

        def one(it, _):
            sweep(step * ITERS + it)
            return 0

        lax.fori_loop(0, ITERS, one, 0)

        @pl.when((step == stages * steps - 1) & down_one)
        def _():
            @pl.when(down_two)
            def _():
                state_copy(0, g - 2).start()

            for side in range(2):
                choose(last, side)

            @pl.when(down_two)
            def _():
                first_send_all(last, 0, g - 2)

            state_copy(1, g - 1).start()
            first_send_all(last, 1, g - 1)

        @pl.when(jnp.logical_not(copied))
        def _():
            weight = weights[n]
            for t in range(tiles):
                r = rows_at(t * TILE)
                for j in range(comp):
                    x = field[j, r, :]
                    levels[n, j, r, :] = x
                    weighted[j, r, :] = weighted[j, r, :] + weight * x
            level_copy(n).start()

        return 0

    def level_if(step, _):
        @pl.when(step < stages * steps)
        def _():
            level(step, 0)

        return 0

    lax.fori_loop(0, 2 * steps, level_if, 0)

    summed = jnp.zeros((nb, cells), jnp.float32)
    for j in range(comp):
        summed = summed + weighted[j] * shape[j]

    mine = lax.dot_general(
        jnp.ones((8, cells), jnp.float32),
        summed,
        (((1,), (1,)), ((), ())),
        precision=lax.Precision.HIGHEST,
        preferred_element_type=jnp.float32,
    )

    def acc_copy(to):
        return pltpu.make_async_remote_copy(
            src_ref=acc_out, dst_ref=acc_in, send_sem=acc_send, recv_sem=acc_recv,
            device_id={"tm": to},
        )

    def total_copy(to):
        return pltpu.make_async_remote_copy(
            src_ref=acc_out, dst_ref=total, send_sem=total_send.at[to], recv_sem=total_recv,
            device_id={"tm": to},
        )

    @pl.when(g == top)
    def _():
        acc_out[...] = mine

    @pl.when(g < top)
    def _():
        acc_copy(g).wait_recv()
        acc_out[...] = mine + acc_in[...]

    @pl.when(g > 0)
    def _():
        acc_copy(g - 1).start()
        total_copy(g).wait_recv()
        sens_ref[...] = total[0:1, :]

    @pl.when(g == 0)
    def _():
        for other in range(1, groups):
            total_copy(other).start()
        sens_ref[...] = acc_out[0:1, :]
        for other in range(1, groups):
            total_copy(other).wait_send()

    @pl.when(g > 0)
    def _():
        acc_copy(g - 1).wait_send()

    @pl.when(copies)
    def _():
        jac_copy(g - 1).wait_send()
        for n in range(steps):
            source_copy(n, g - 1).wait_send()

    @pl.when(has_across)
    def _():
        fixed_copy().wait_send()
        rate_copy(0).wait_send()

        @pl.when(twice)
        def _():
            rate_copy(1).wait_send()

    @pl.when(g == top)
    def _():
        first_drain(-1, 0, g)

    @pl.when(down_two)
    def _():
        state_copy(0, g - 2).wait_send()
        first_drain(last, 0, g - 2)

    @pl.when(down_one)
    def _():
        state_copy(1, g - 1).wait_send()
        first_drain(last, 1, g - 1)

    def drain(slot, _):
        @pl.when(slot < last)
        def _():
            partner_copy(slot).wait_send()

        @pl.when(has_beyond & (slot < last - 1))
        def _():
            second_copy(slot, beyond).wait_send()

        @pl.when(has_across & (slot < last))
        def _():
            across_copy(slot).wait_send()

        return 0

    lax.fori_loop(1, 2 * sweeps, drain, 0)
    for n in range(steps):
        level_copy(n).wait()


def per_device(groups, width, *args):
    (source, terminal, jacobian, face_coef, cell_coef, neighbours, send_blocks,
     live_count, volume, shape_field, weights) = args
    steps, nb, comp, cells = source.shape
    nei = face_coef.shape[1]
    count = send_blocks.shape[2]
    edges = 2 * count
    slots = 2 * steps * ITERS
    f32 = jnp.float32
    bf16 = jnp.bfloat16
    hbm = pl.BlockSpec(memory_space=pltpu.MemorySpace.HBM)
    smem = pl.BlockSpec(memory_space=pltpu.SMEM)
    vmem = pltpu.VMEM
    dma = pltpu.SemaphoreType.DMA
    block = (comp, nb, cells)
    flat = comp * cells
    edge = (comp, count, cells)
    adjoint, sens = pl.pallas_call(
        functools.partial(kernel, groups, width),
        out_shape=(
            jax.ShapeDtypeStruct((steps, comp, nb, cells), f32),
            jax.ShapeDtypeStruct((1, nb), f32),
        ),
        in_specs=[hbm, hbm, hbm, hbm, hbm, hbm, smem, smem, hbm, hbm, smem],
        out_specs=(hbm, pl.BlockSpec(memory_space=pltpu.VMEM)),
        scratch_shapes=[
            vmem((2, steps, comp, nb, cells), f32),
            vmem(block, f32),
            vmem((2, comp, comp, nb, cells), f32),
            vmem((nei, nb, cells), f32),
            vmem((nb, cells), f32),
            vmem((nei, nb), jnp.int32),
            vmem((nb, cells), f32),
            vmem(block, f32),
            vmem(block, f32),
            vmem(block, f32),
            vmem((2,) + block, f32),
            vmem((2,) + block, f32),
            vmem((nb, cells), f32),
            vmem((nb, cells), f32),
            vmem(block, f32),
            vmem((steps, comp, nb, cells), f32),
            vmem(block, f32),
            vmem((nei * nb, 2 * nb), bf16),
            vmem((nei * nb, nb), bf16),
            vmem((2 * nb, flat), bf16),
            vmem((nb, flat), bf16),
            vmem((nb, flat), bf16),
            vmem((nei * nb, flat), f32),
            vmem((nei * nb, flat), f32),
            vmem((count, nb), f32),
            vmem((2 * nei, count, cells), f32),
            vmem((2,) + edge, f32),
            vmem((2 * nei, count, cells), f32),
            vmem((2,) + edge, f32),
            vmem((nei * count, nb), bf16),
            vmem(edge, f32),
            vmem((slots + 1,) + edge, f32),
            vmem((slots + 1,) + edge, f32),
            vmem((slots + 1,) + edge, f32),
            vmem((slots + 2, 2) + edge, f32),
            vmem((slots + 1,) + edge, f32),
            vmem((8, nb), f32),
            vmem((8, nb), f32),
            vmem((8, nb), f32),
            dma((8,)),
            dma((steps,)),
            dma((1 + steps,)),
            dma((1 + steps,)),
            dma((3,)),
            dma((3,)),
            dma((slots + 1,)),
            dma((slots + 1,)),
            dma((slots + 1,)),
            dma((slots + 1,)),
            dma((slots + 1,)),
            dma((slots + 1,)),
            dma((2, 3)),
            dma((2,)),
            dma,
            dma,
            dma,
            dma((groups,)),
            dma,
        ],
        compiler_params=pltpu.CompilerParams(collective_id=0, has_side_effects=True),
    )(
        source.transpose(0, 2, 1, 3),
        terminal.transpose(1, 0, 2),
        jacobian.transpose(0, 2, 3, 1, 4),
        face_coef.transpose(1, 0, 2),
        cell_coef,
        neighbours.T,
        send_blocks,
        live_count,
        volume,
        shape_field.transpose(1, 0, 2),
        weights,
    )
    return adjoint.transpose(0, 2, 1, 3), sens.reshape(nb)


def solution(mesh):
    sizes = dict(mesh.shape)
    return jax.shard_map(
        functools.partial(per_device, sizes["tm"], sizes["space"]),
        mesh=mesh,
        in_specs=(
            P("tm", "space", None, None),
            P("space", None, None),
            P("tm", "space", None, None, None),
            P("space", None, None),
            P("space", None),
            P("space", None),
            P("space", None, None),
            P("space"),
            P("space", None),
            P("space", None, None),
            P("tm"),
        ),
        out_specs=(P("tm", "space", None, None), P("space")),
        check_vma=False,
    )
```

```python
import functools

import jax
import jax.numpy as jnp
from jax import lax
from jax.experimental import pallas as pl
from jax.experimental.pallas import tpu as pltpu
from jax.sharding import PartitionSpec as P

ITERS = 3
INVERSE_STEP = 6.0
TILE = 16


def rows_at(start):
    return pl.ds(start if isinstance(start, int) else pl.multiple_of(start, TILE), TILE)


def split(x):
    high = x.astype(jnp.bfloat16)
    return high, (x - high.astype(jnp.float32)).astype(jnp.bfloat16)


def matmul(a, b):
    return jnp.dot(a, b, preferred_element_type=jnp.float32)


def kernel(
    groups,
    width,
    source_hbm,
    terminal_hbm,
    jac_hbm,
    face_hbm,
    cell_hbm,
    nbr_hbm,
    send_blocks,
    live_count,
    volume_hbm,
    shape_hbm,
    weights,
    adjoint_hbm,
    sens_ref,
    source,
    terminal,
    jac,
    face,
    cell,
    nbr,
    volume,
    shape,
    field,
    part,
    rate,
    rate_mass,
    cell_left,
    cell_right,
    rhs,
    levels,
    weighted,
    near_pick,
    far_pick,
    field_terms,
    halo_terms,
    edge_terms,
    near,
    far,
    select,
    own_fixed,
    own_rate,
    their_fixed,
    their_rate,
    their_pick,
    edge_halo,
    from_partner,
    from_across,
    from_second,
    edge_out,
    part_out,
    acc_in,
    acc_out,
    total,
    load_sem,
    store_sem,
    copy_send,
    copy_recv,
    coef_send,
    coef_recv,
    partner_send,
    partner_recv,
    across_send,
    across_recv,
    second_send,
    second_recv,
    first_send,
    state_send,
    state_recv,
    acc_send,
    acc_recv,
    total_send,
    total_recv,
):
    g = lax.axis_index("tm")
    d = lax.axis_index("space")
    _, steps, comp, nb, cells = source.shape
    nei = face.shape[0]
    count = edge_out.shape[3]
    sweeps = steps * ITERS
    tiles = nb // TILE
    edges = 2 * count
    top = groups - 1

    odd = lax.rem(d, 2)
    partner = d + 1 - 2 * odd
    across = d - 1 + 2 * odd
    beyond = d + 2 - 4 * odd
    second = d - 2 + 4 * odd
    has_across = (across >= 0) & (across < width)
    has_beyond = (beyond >= 0) & (beyond < width)

    even = lax.rem(g, 2) == 0
    down_two = even & (g > 1)
    down_one = down_two | (g == top)
    copies = (lax.rem(g, 2) == 1) & (g < top)
    twice = (lax.rem(g, 2) == 0) & (g + 1 < top)
    stages = jnp.where(twice, 2, 1)
    last = stages * sweeps

    loads = [
        pltpu.make_async_copy(nbr_hbm, nbr, load_sem.at[0]),
        pltpu.make_async_copy(face_hbm, face, load_sem.at[1]),
        pltpu.make_async_copy(cell_hbm, cell, load_sem.at[2]),
        pltpu.make_async_copy(volume_hbm, volume, load_sem.at[3]),
        pltpu.make_async_copy(jac_hbm.at[0], jac.at[0], load_sem.at[4]),
        pltpu.make_async_copy(terminal_hbm, terminal, load_sem.at[5]),
        pltpu.make_async_copy(source_hbm, source.at[0], load_sem.at[6]),
        pltpu.make_async_copy(shape_hbm, shape, load_sem.at[7]),
    ]
    for load in loads:
        load.start()

    @pl.when(jnp.logical_not(has_across))
    def _():
        from_across[...] = jnp.zeros_like(from_across)

    barrier = pltpu.get_barrier_semaphore()
    for other in range(groups):
        @pl.when(g != other)
        def _():
            pl.semaphore_signal(barrier, inc=1, device_id={"tm": other})

    up_two = even & (g + 2 < groups)
    up_one = (jnp.logical_not(even) & (g + 1 < groups)) | (g + 1 == top)

    def greet(side):
        pl.semaphore_signal(barrier, inc=1, device_id={"space": side})
        for shift, linked in ((-2, down_two), (-1, down_one), (1, up_one), (2, up_two)):
            @pl.when(linked)
            def _():
                pl.semaphore_signal(barrier, inc=1, device_id={"tm": g + shift, "space": side})

    for shift in (1, 2):
        @pl.when(d > shift - 1)
        def _():
            greet(d - shift)

        @pl.when(d < width - shift)
        def _():
            greet(d + shift)

    sides = sum(jnp.where(d > i - 1, 1, 0) + jnp.where(d < width - i, 1, 0) for i in (1, 2))
    slabs = 1 + sum(jnp.where(linked, 1, 0) for linked in (down_two, down_one, up_one, up_two))
    expected = groups - 1 + sides * slabs

    def jac_copy(to):
        return pltpu.make_async_remote_copy(
            src_ref=jac_hbm.at[0], dst_ref=jac.at[1], send_sem=copy_send.at[0],
            recv_sem=copy_recv.at[0], device_id={"tm": to},
        )

    def source_copy(n, to):
        return pltpu.make_async_remote_copy(
            src_ref=source_hbm.at[n], dst_ref=source.at[1, n], send_sem=copy_send.at[1 + n],
            recv_sem=copy_recv.at[1 + n], device_id={"tm": to},
        )

    @pl.when(copies)
    def _():
        pl.semaphore_wait(barrier, expected)
        jac_copy(g - 1).start()
        for n in reversed(range(steps)):
            source_copy(n, g - 1).start()

    def block_of(side, s):
        return jnp.where(odd == side, send_blocks[0, 1, s], send_blocks[0, 0, s])

    halo_terms[...] = jnp.zeros_like(halo_terms)
    edge_terms[...] = jnp.zeros_like(edge_terms)
    edge_halo[...] = jnp.zeros_like(edge_halo)
    lane = lax.broadcasted_iota(jnp.int32, (1, nb), 1)
    for s in range(count):
        select[pl.ds(s, 1), :] = jnp.where(lane == block_of(1, s), 1.0, 0.0)
    chosen = select[...].astype(jnp.bfloat16)

    loads[0].wait()
    listed = nbr[...].astype(jnp.float32)
    listed = jnp.concatenate([listed, jnp.zeros((nb - nei, nb), jnp.float32)], axis=0).T
    wide = lax.broadcasted_iota(jnp.int32, (nb, nb), 1).astype(jnp.float32)
    swap = ((1 - odd) * count).astype(jnp.float32)
    for k in range(nei):
        column = jnp.broadcast_to(listed[:, k : k + 1], (nb, nb))
        pick = jnp.where(column == wide, 1.0, 0.0).astype(jnp.bfloat16)
        near_pick[pl.ds(k * nb, nb), :nb] = pick
        near_pick[pl.ds(k * nb, nb), nb:] = pick
        shifted = column - nb
        inside = (shifted >= 0) & (shifted < edges)
        shifted = shifted + swap * jnp.where(shifted < count, 1.0, -1.0)
        hit = (shifted == wide) | (shifted + edges == wide)
        pick = jnp.where(hit & inside, 1.0, 0.0).astype(jnp.bfloat16)
        far_pick[pl.ds(k * nb, nb), :] = pick
        own_fixed[k] = matmul(chosen, pick)

    for load in loads[1:5]:
        load.wait()
    alive = live_count[0]
    row_id = lax.broadcasted_iota(jnp.int32, (TILE, cells), 0)
    lane_id = lax.broadcasted_iota(jnp.int32, (TILE, cells), 1)

    def live_of(t):
        return jnp.where(row_id + t * TILE < alive, 1.0, 0.0)

    def prepare(t, store):
        r = rows_at(t * TILE)
        live = live_of(t)
        mass = INVERSE_STEP * volume[r, :]
        along = cell[r, :]
        base = mass + 2.0 * along
        for k in range(nei):
            base = base + face[k, r, :]
        if store == 0:
            cell_left[r, :] = jnp.where(lane_id == 0, 0.0, along)
            cell_right[r, :] = jnp.where(lane_id == cells - 1, 0.0, along)
        for j in range(comp):
            c = live / (base + jac[store, j, j, r, :])
            rate[store, j, r, :] = c
            drift = c * mass
            rate_mass[store, j, r, :] = drift
            for i in range(comp):
                entry = -c * jac[store, i, j, r, :]
                jac[store, i, j, r, :] = entry + (live - drift) if i == j else entry
            if store == 0:
                weighted[j, r, :] = jnp.zeros((TILE, cells), jnp.float32)

    def fixed_copy():
        return pltpu.make_async_remote_copy(
            src_ref=own_fixed, dst_ref=their_fixed, send_sem=coef_send.at[0],
            recv_sem=coef_recv.at[0], device_id={"space": across},
        )

    def rate_copy(store):
        return pltpu.make_async_remote_copy(
            src_ref=own_rate.at[store], dst_ref=their_rate.at[store], send_sem=coef_send.at[1 + store],
            recv_sem=coef_recv.at[1 + store], device_id={"space": across},
        )

    for t in range(tiles):
        prepare(t, 0)
    for s in range(count):
        block = pl.ds(block_of(1, s), 1)
        for k in range(nei):
            own_fixed[nei + k, pl.ds(s, 1), :] = face[k, block, :]
        for j in range(comp):
            own_rate[0, j, pl.ds(s, 1), :] = rate[0, j, block, :]

    for load in loads[5:]:
        load.wait()

    @pl.when(jnp.logical_not(copies))
    def _():
        pl.semaphore_wait(barrier, expected)

    def lanes(j):
        return slice(j * cells, (j + 1) * cells)

    def put_terms(ref, t, j, x):
        high, low = split(x)
        ref[rows_at(t * TILE), lanes(j)] = high
        ref[rows_at(nb + t * TILE), lanes(j)] = low

    def put_edges(ref, side, j, x):
        high, low = split(x)
        ref[side * count : (side + 1) * count, lanes(j)] = high
        ref[edges + side * count : edges + (side + 1) * count, lanes(j)] = low

    def state_copy(way, to):
        return pltpu.make_async_remote_copy(
            src_ref=field, dst_ref=field, send_sem=state_send.at[way], recv_sem=state_recv,
            device_id={"tm": to},
        )

    def partner_copy(slot):
        return pltpu.make_async_remote_copy(
            src_ref=edge_out.at[slot + 1, 0], dst_ref=from_partner.at[slot],
            send_sem=partner_send.at[slot], recv_sem=partner_recv.at[slot],
            device_id={"space": partner},
        )

    def second_copy(slot, to):
        return pltpu.make_async_remote_copy(
            src_ref=edge_out.at[slot + 1, 0], dst_ref=from_second.at[slot + 1],
            send_sem=second_send.at[slot + 1], recv_sem=second_recv.at[slot + 1],
            device_id={"space": to},
        )

    def across_copy(slot):
        return pltpu.make_async_remote_copy(
            src_ref=part_out.at[slot], dst_ref=from_across.at[slot],
            send_sem=across_send.at[slot], recv_sem=across_recv.at[slot],
            device_id={"space": across},
        )

    def first_copies(slot, way, to):
        kinds = ((0, partner, from_partner.at[0], partner_recv.at[0]),
                 (1, across, from_across.at[0], across_recv.at[0]),
                 (0, beyond, from_second.at[1], second_recv.at[1]))
        return [
            pltpu.make_async_remote_copy(
                src_ref=edge_out.at[slot + 1, side], dst_ref=ref,
                send_sem=first_send.at[way, i], recv_sem=recv,
                device_id={"tm": to, "space": place},
            )
            for i, (side, place, ref, recv) in enumerate(kinds)
        ]

    def first_send_all(slot, way, to):
        near_one, across_one, second_one = first_copies(slot, way, to)

        @pl.when(has_across)
        def _():
            across_one.start()

        @pl.when(has_beyond)
        def _():
            second_one.start()

        near_one.start()

    def first_drain(slot, way, to):
        near_one, across_one, second_one = first_copies(slot, way, to)

        @pl.when(has_across)
        def _():
            across_one.wait_send()

        @pl.when(has_beyond)
        def _():
            second_one.wait_send()

        near_one.wait_send()

    def choose(slot, side):
        for s in range(count):
            for j in range(comp):
                edge_out[slot + 1, side, j, pl.ds(s, 1), :] = field[j, pl.ds(block_of(side, s), 1), :]

    @pl.when(g == top)
    def _():
        for t in range(tiles):
            r = rows_at(t * TILE)
            for j in range(comp):
                x = live_of(t) * terminal[j, r, :]
                field[j, r, :] = x
                put_terms(field_terms, t, j, x)
        for side in range(2):
            choose(-1, side)
        first_send_all(-1, 0, g)

    @pl.when(has_across)
    def _():
        fixed_copy().start()
        rate_copy(0).start()

    @pl.when(twice)
    def _():
        jac_copy(g).wait_recv()
        for t in range(tiles):
            prepare(t, 1)
        for s in range(count):
            for j in range(comp):
                own_rate[1, j, pl.ds(s, 1), :] = rate[1, j, pl.ds(block_of(1, s), 1), :]

        @pl.when(has_across)
        def _():
            rate_copy(1).start()

    @pl.when(g < top)
    def _():
        state_copy(0, g).wait_recv()
        for t in range(tiles):
            for j in range(comp):
                put_terms(field_terms, t, j, field[j, rows_at(t * TILE), :])

    def sweep(m):
        store = jnp.where(twice & (m < sweeps), 1, 0)
        near[...] = matmul(near_pick[...], field_terms[...])

        for t in range(tiles):
            r = rows_at(t * TILE)
            x = [field[i, r, :] for i in range(comp)]
            left = cell_left[r, :]
            right = cell_right[r, :]
            for j in range(comp):
                value = left * pltpu.roll(x[j], 1, 1) + right * pltpu.roll(x[j], cells - 1, 1)
                for k in range(nei):
                    q = rows_at(k * nb + t * TILE)
                    value = value + face[k, r, :] * near[q, lanes(j)]
                value = rhs[j, r, :] + rate[store, j, r, :] * value
                for i in range(comp):
                    value = value + jac[store, i, j, r, :] * x[i]
                part[j, r, :] = value

        @pl.when(has_across & (m < last - 1))
        def _():
            for s in range(count):
                for j in range(comp):
                    part_out[m + 1, j, pl.ds(s, 1), :] = part[j, pl.ds(block_of(1, s), 1), :]
            across_copy(m + 1).start()

        choose(m, 1)

        @pl.when(has_across & (m == 1))
        def _():
            fixed_copy().wait_recv()
            rate_copy(0).wait_recv()
            for k in range(nei):
                their_pick[k * count : (k + 1) * count, :] = their_fixed[k].astype(jnp.bfloat16)

            @pl.when(twice)
            def _():
                rate_copy(1).wait_recv()

        @pl.when(has_across & (m > 0))
        def _():
            kept = jnp.where(twice & (m <= sweeps), 1, 0)
            second_copy(m - 1, second).wait_recv()
            for side in range(2):
                for j in range(comp):
                    put_edges(edge_terms, side, j, from_second[m, j] if side == 0 else edge_out[m, 1, j])
            arrived = matmul(their_pick[...], edge_terms[...])
            for j in range(comp):
                value = None
                for k in range(nei):
                    term = their_fixed[nei + k] * arrived[k * count : (k + 1) * count, lanes(j)]
                    value = term if value is None else value + term
                edge_halo[j] = their_rate[kept, j] * value

        partner_copy(m).wait_recv()
        for j in range(comp):
            put_edges(halo_terms, 0, j, from_partner[m, j])

        @pl.when(has_across)
        def _():
            across_copy(m).wait_recv()

        for j in range(comp):
            put_edges(halo_terms, 1, j, from_across[m, j] + edge_halo[j])

        far[...] = matmul(far_pick[...], halo_terms[...])

        for t in range(tiles):
            r = rows_at(t * TILE)
            faces = [face[k, r, :] for k in range(nei)]
            for j in range(comp):
                value = None
                for k in range(nei):
                    q = rows_at(k * nb + t * TILE)
                    term = faces[k] * far[q, lanes(j)]
                    value = term if value is None else value + term
                value = part[j, r, :] + rate[store, j, r, :] * value
                field[j, r, :] = value
                put_terms(field_terms, t, j, value)

        @pl.when(m < last - 1)
        def _():
            choose(m + 1, 0)
            partner_copy(m + 1).start()

            @pl.when(has_beyond & (m < last - 2))
            def _():
                second_copy(m + 1, beyond).start()

    def level_copy(n):
        return pltpu.make_async_copy(levels.at[n], adjoint_hbm.at[n], store_sem.at[n])

    def level(step, _):
        copied = twice & (step < steps)
        store = jnp.where(copied, 1, 0)
        n = steps - 1 - lax.rem(step, steps)

        @pl.when(copied)
        def _():
            source_copy(n, g).wait_recv()

        for t in range(tiles):
            r = rows_at(t * TILE)
            for j in range(comp):
                rhs[j, r, :] = (
                    rate[store, j, r, :] * source[store, n, j, r, :] + rate_mass[store, j, r, :] * field[j, r, :]
                )

        def one(it, _):
            sweep(step * ITERS + it)
            return 0

        lax.fori_loop(0, ITERS, one, 0)

        @pl.when((step == stages * steps - 1) & down_one)
        def _():
            @pl.when(down_two)
            def _():
                state_copy(0, g - 2).start()

            for side in range(2):
                choose(last, side)

            @pl.when(down_two)
            def _():
                first_send_all(last, 0, g - 2)

            state_copy(1, g - 1).start()
            first_send_all(last, 1, g - 1)

        @pl.when(jnp.logical_not(copied))
        def _():
            weight = weights[n]
            for t in range(tiles):
                r = rows_at(t * TILE)
                for j in range(comp):
                    x = field[j, r, :]
                    levels[n, j, r, :] = x
                    weighted[j, r, :] = weighted[j, r, :] + weight * x
            level_copy(n).start()

        return 0

    def level_if(step, _):
        @pl.when(step < stages * steps)
        def _():
            level(step, 0)

        return 0

    lax.fori_loop(0, 2 * steps, level_if, 0)

    summed = jnp.zeros((nb, cells), jnp.float32)
    for j in range(comp):
        summed = summed + weighted[j] * shape[j]

    mine = lax.dot_general(
        jnp.ones((8, cells), jnp.float32),
        summed,
        (((1,), (1,)), ((), ())),
        precision=lax.Precision.HIGHEST,
        preferred_element_type=jnp.float32,
    )

    def acc_copy(to):
        return pltpu.make_async_remote_copy(
            src_ref=acc_out, dst_ref=acc_in, send_sem=acc_send, recv_sem=acc_recv,
            device_id={"tm": to},
        )

    def total_copy(to):
        return pltpu.make_async_remote_copy(
            src_ref=acc_out, dst_ref=total, send_sem=total_send.at[to], recv_sem=total_recv,
            device_id={"tm": to},
        )

    @pl.when(g == top)
    def _():
        acc_out[...] = mine

    @pl.when(g < top)
    def _():
        acc_copy(g).wait_recv()
        acc_out[...] = mine + acc_in[...]

    @pl.when(g > 0)
    def _():
        acc_copy(g - 1).start()
        total_copy(g).wait_recv()
        sens_ref[...] = total[0:1, :]

    @pl.when(g == 0)
    def _():
        for other in range(1, groups):
            total_copy(other).start()
        sens_ref[...] = acc_out[0:1, :]
        for other in range(1, groups):
            total_copy(other).wait_send()

    @pl.when(g > 0)
    def _():
        acc_copy(g - 1).wait_send()

    @pl.when(copies)
    def _():
        jac_copy(g - 1).wait_send()
        for n in range(steps):
            source_copy(n, g - 1).wait_send()

    @pl.when(has_across)
    def _():
        fixed_copy().wait_send()
        rate_copy(0).wait_send()

        @pl.when(twice)
        def _():
            rate_copy(1).wait_send()

    @pl.when(g == top)
    def _():
        first_drain(-1, 0, g)

    @pl.when(down_two)
    def _():
        state_copy(0, g - 2).wait_send()
        first_drain(last, 0, g - 2)

    @pl.when(down_one)
    def _():
        state_copy(1, g - 1).wait_send()
        first_drain(last, 1, g - 1)

    def drain(slot, _):
        @pl.when(slot < last)
        def _():
            partner_copy(slot).wait_send()

        @pl.when(has_beyond & (slot < last - 1))
        def _():
            second_copy(slot, beyond).wait_send()

        @pl.when(has_across & (slot < last))
        def _():
            across_copy(slot).wait_send()

        return 0

    lax.fori_loop(1, 2 * sweeps, drain, 0)
    for n in range(steps):
        level_copy(n).wait()


def per_device(groups, width, *args):
    (source, terminal, jacobian, face_coef, cell_coef, neighbours, send_blocks,
     live_count, volume, shape_field, weights) = args
    steps, nb, comp, cells = source.shape
    nei = face_coef.shape[1]
    count = send_blocks.shape[2]
    edges = 2 * count
    slots = 2 * steps * ITERS
    f32 = jnp.float32
    bf16 = jnp.bfloat16
    hbm = pl.BlockSpec(memory_space=pltpu.MemorySpace.HBM)
    smem = pl.BlockSpec(memory_space=pltpu.SMEM)
    vmem = pltpu.VMEM
    dma = pltpu.SemaphoreType.DMA
    block = (comp, nb, cells)
    flat = comp * cells
    edge = (comp, count, cells)
    adjoint, sens = pl.pallas_call(
        functools.partial(kernel, groups, width),
        out_shape=(
            jax.ShapeDtypeStruct((steps, comp, nb, cells), f32),
            jax.ShapeDtypeStruct((1, nb), f32),
        ),
        in_specs=[hbm, hbm, hbm, hbm, hbm, hbm, smem, smem, hbm, hbm, smem],
        out_specs=(hbm, pl.BlockSpec(memory_space=pltpu.VMEM)),
        scratch_shapes=[
            vmem((2, steps, comp, nb, cells), f32),
            vmem(block, f32),
            vmem((2, comp, comp, nb, cells), f32),
            vmem((nei, nb, cells), f32),
            vmem((nb, cells), f32),
            vmem((nei, nb), jnp.int32),
            vmem((nb, cells), f32),
            vmem(block, f32),
            vmem(block, f32),
            vmem(block, f32),
            vmem((2,) + block, f32),
            vmem((2,) + block, f32),
            vmem((nb, cells), f32),
            vmem((nb, cells), f32),
            vmem(block, f32),
            vmem((steps, comp, nb, cells), f32),
            vmem(block, f32),
            vmem((nei * nb, 2 * nb), bf16),
            vmem((nei * nb, nb), bf16),
            vmem((2 * nb, flat), bf16),
            vmem((nb, flat), bf16),
            vmem((nb, flat), bf16),
            vmem((nei * nb, flat), f32),
            vmem((nei * nb, flat), f32),
            vmem((count, nb), f32),
            vmem((2 * nei, count, cells), f32),
            vmem((2,) + edge, f32),
            vmem((2 * nei, count, cells), f32),
            vmem((2,) + edge, f32),
            vmem((nei * count, nb), bf16),
            vmem(edge, f32),
            vmem((slots + 2,) + edge, f32),
            vmem((slots + 2,) + edge, f32),
            vmem((slots + 2,) + edge, f32),
            vmem((slots + 2, 2) + edge, f32),
            vmem((slots + 2,) + edge, f32),
            vmem((8, nb), f32),
            vmem((8, nb), f32),
            vmem((8, nb), f32),
            dma((8,)),
            dma((steps,)),
            dma((1 + steps,)),
            dma((1 + steps,)),
            dma((3,)),
            dma((3,)),
            dma((slots + 2,)),
            dma((slots + 2,)),
            dma((slots + 2,)),
            dma((slots + 2,)),
            dma((slots + 2,)),
            dma((slots + 2,)),
            dma((2, 3)),
            dma((2,)),
            dma,
            dma,
            dma,
            dma((groups,)),
            dma,
        ],
        compiler_params=pltpu.CompilerParams(collective_id=0, has_side_effects=True),
    )(
        source.transpose(0, 2, 1, 3),
        terminal.transpose(1, 0, 2),
        jacobian.transpose(0, 2, 3, 1, 4),
        face_coef.transpose(1, 0, 2),
        cell_coef,
        neighbours.T,
        send_blocks,
        live_count,
        volume,
        shape_field.transpose(1, 0, 2),
        weights,
    )
    return adjoint.transpose(0, 2, 1, 3), sens.reshape(nb)


def solution(mesh):
    sizes = dict(mesh.shape)
    return jax.shard_map(
        functools.partial(per_device, sizes["tm"], sizes["space"]),
        mesh=mesh,
        in_specs=(
            P("tm", "space", None, None),
            P("space", None, None),
            P("tm", "space", None, None, None),
            P("space", None, None),
            P("space", None),
            P("space", None),
            P("space", None, None),
            P("space"),
            P("space", None),
            P("space", None, None),
            P("tm"),
        ),
        out_specs=(P("tm", "space", None, None), P("space")),
        check_vma=False,
    )
```
